32 devices in a mesh: gx: 4 (over x, core), gy: 2 (over y), gz: 4 (over z).
Axes of the slice: x: 2, y: 2, z: 4, core: 2. Of those that a mesh axis runs over, the one named last changes fastest.
Arguments:
- velocity: float32 [3, 128, 192, 1024], P(None, 'gx', 'gy', 'gz'), may hold values from -6 to 6
Outputs:
- magnitude: float32 [128, 192, 1024], P('gx', ('gy', 'gz'))
- level_one: float32 [64, 96, 512], P('gx', 'gy')
- level_two: float32 [32, 48, 256], P('gx', 'gy')
- level_three: float32 [16, 24, 128], P('gx', 'gy')
- level_four: float32 [8, 12, 64], P('gx', 'gy')
- level_five: float32 [4, 6, 32], P('gx', 'gy')
The draws below stay inside these ranges and needn't reach their ends.
All inputs are finite; a program needn't handle non-finite values.
Results may differ from the reference program's by a relative error of at most 0.000075.
Values sent between devices are 32-bit elements; how exact they have to be, the bound alone decides.
A program may use at most 256 MiB of HBM per device.

```python
import jax
import jax.numpy as jnp
from jax import lax

NX = 128
NY = 192
NZ = 1024


def shard_levels(stream_key, extent, cuts, least, top_value):
    loudness, own = 1.0, jax.random.fold_in(stream_key, 6)
    for axis_at, blocks in cuts:
        steps = jnp.exp(jax.random.uniform(jax.random.fold_in(own, axis_at), (blocks,), jnp.float32, least / len(cuts), top_value / len(cuts)))
        loudness = loudness * jnp.repeat(steps, extent[axis_at] // blocks).reshape([-1 if axis == axis_at else 1 for axis in range(len(extent))])
    return loudness


def normal_values(own_key, extent, scale, limit, split=(), held_as=jnp.bfloat16):
    level = shard_levels(own_key, extent, split, -0.22, 0.18) if split else 1.0
    array = jax.random.normal(own_key, extent, jnp.float32) * scale * level
    return jnp.minimum(jnp.maximum(array, -limit), limit).astype(held_as)


def setup_inputs(seed: int = 0) -> dict:
    streams_of = jax.random.split(jax.random.key(seed), 2)
    velocity = normal_values(streams_of[0], (3, NX, NY, NZ), 1.0, 6.0, ((1, 4), (2, 2), (3, 4)), jnp.float32)
    return {"velocity": velocity}


def central(field, axis):
    return (jnp.roll(field, -1, axis) - jnp.roll(field, 1, axis)) * 0.5

def pooled(field):
    rows, cols, depth = field.shape
    blocks = field.reshape(rows // 2, 2, cols // 2, 2, depth // 2, 2)
    return lax.optimization_barrier(jnp.mean(blocks, axis=(1, 3, 5)))

def reference(velocity):
    speed_u = velocity[0]
    speed_v = velocity[1]
    speed_w = velocity[2]
    curl_first = central(speed_w, 1) - central(speed_v, 2)
    curl_second = central(speed_u, 2) - central(speed_w, 0)
    curl_third = central(speed_v, 0) - central(speed_u, 1)
    magnitude = jnp.sqrt(1.0 + curl_first * curl_first + curl_second * curl_second + curl_third * curl_third)
    level_one = pooled(magnitude)
    level_two = pooled(level_one)
    level_three = pooled(level_two)
    level_four = pooled(level_three)
    level_five = pooled(level_four)
    return (magnitude, level_one, level_two, level_three, level_four, level_five)
```

```python
import functools

import jax
import jax.numpy as jnp
from jax import lax
from jax.experimental import pallas as pl
from jax.experimental.pallas import tpu as pltpu
from jax.sharding import PartitionSpec as P

MESH = pl.DeviceIdType.MESH
LANES = 128
CHUNKS = 4
ORDER = (1, 2, 3, 0)
LOAD_ORDER = (1, 2, 0, 3)
MIB = 1024 * 1024


def remote(src, dst, send, recv, device):
    return pltpu.make_async_remote_copy(
        src_ref=src, dst_ref=dst, send_sem=send, recv_sem=recv, device_id=device, device_id_type=MESH
    )


def halve_lanes(rows):
    depth = rows.shape[1]
    fine = lax.broadcasted_iota(jnp.int32, (depth, depth // 2), 0)
    coarse = lax.broadcasted_iota(jnp.int32, (depth, depth // 2), 1)
    weight = jnp.where(fine // 2 == coarse, 0.125, 0.0).astype(jnp.bfloat16)
    high = rows.astype(jnp.bfloat16)
    rest = rows - high.astype(jnp.float32)
    low = rest.astype(jnp.bfloat16)
    last = (rest - low.astype(jnp.float32)).astype(jnp.bfloat16)

    def dot(a):
        return jnp.dot(a, weight, preferred_element_type=jnp.float32)

    return dot(high) + (dot(low) + dot(last))


def pooled(read, count, size, work):
    tiles = work.shape[0]
    for i in range(count):
        value = read(2 * i) + read(2 * i + 1)
        depth = value.shape[1]
        for t in range(tiles):
            wide = min(LANES, depth - t * LANES)
            work[t, i * size:(i + 1) * size, :wide] = value[:, t * LANES:t * LANES + wide]
    lines = count * size // 2
    parts = [
        work[t, pl.ds(0, lines, stride=2), :] + work[t, pl.ds(1, lines, stride=2), :] for t in range(tiles)]
    return halve_lanes(jnp.concatenate(parts, axis=1)[:, :depth])


def carries(n, j, up, q, s):
    low, high = min(q, s), max(q, s)
    if up:
        return j < n - 1 and (high <= j or (low <= j and high > j + 1 and 2 * (j + 1) < n))
    return j > 0 and (low >= j or (high >= j and low < j - 1 and 2 * (j - 1) >= n))


def blocks(n):
    return [(q, s) for q in range(n) for s in range(n)]


def mag_time(n, s, q, k):
    d = abs(s - q)
    if s in (0, n - 1):
        return 4 * (k + 1) if d == 1 else 20 + 14 * (k + (d - 1) / (n - 2))
    outward = q < s if 2 * s < n else q > s
    return 4 * k + 6 if outward else 12 * (k + d / n)


def events(n, me):
    @functools.lru_cache(None)
    def ready(j, q, s, k):
        if j == s:
            return 0.0
        if j == q:
            return mag_time(n, s, q, k)
        for i, up in ((j - 1, True), (j + 1, False)):
            if 0 <= i < n and carries(n, i, up, q, s):
                crossing = 2 * (i + 1) == n if up else 2 * i == n
                return max(ready(i, q, s, k), (50 if crossing else 20) + 2 * k) + 3
        raise ValueError((j, q, s))

    found = []
    for k in range(CHUNKS):
        for q, s in blocks(n):
            if s != me:
                found.append((ready(me, q, s, k), q, s, k))
    return sorted(found)


def kernel(
    sizes, vel_hbm, pencil, one,
    vel, ypack, yhalo, zpack, zhalo, zside, stage, piece, work,
    load_sem, xs_sem, xr_sem, ys_sem, yr_sem, zs_sem, zr_sem, as_sem, ar_sem, move_sem, piece_sem,
):
    nx, ny, nz = sizes
    gx, gy, me = lax.axis_index("gx"), lax.axis_index("gy"), lax.axis_index("gz")
    _, planes, cols, depth = vel_hbm.shape
    rows = cols // nz
    half = depth // 2
    step = planes // CHUNKS
    pairs = step // 2
    group = pairs * rows // 2
    f32 = jnp.float32

    def at(dx=0, dy=0, dz=0):
        return (lax.rem(gx + dx + nx, nx), lax.rem(gy + dy + ny, ny), lax.rem(me + dz + nz, nz))

    barrier = pltpu.get_barrier_semaphore()
    friends = [at(dx=1), at(dx=-1), at(dy=1), at(dy=-1)] + [at(dz=d) for d in range(1, nz)]
    for friend in friends:
        pl.semaphore_signal(barrier, inc=1, device_id=friend, device_id_type=MESH)

    loads = {}
    for k in LOAD_ORDER:
        loads[k] = pltpu.make_async_copy(
            vel_hbm.at[:, pl.ds(k * step, step)], vel.at[:, pl.ds(1 + k * step, step)], load_sem.at[k])
        loads[k].start()
    pl.semaphore_wait(barrier, len(friends))

    xcopies = [
        remote(vel_hbm.at[pl.ds(1, 2), planes - 1], vel.at[pl.ds(1, 2), 0], xs_sem.at[0], xr_sem.at[0], at(dx=1)),
        remote(vel_hbm.at[pl.ds(1, 2), 0], vel.at[pl.ds(1, 2), planes + 1], xs_sem.at[1], xr_sem.at[1], at(dx=-1)),
    ]
    for copy in xcopies:
        copy.start()

    lane = lax.broadcasted_iota(jnp.int32, (cols, LANES), 1)
    sides = {}
    for k in ORDER:
        def pack(i, carry):
            first, last = carry
            x = k * step + i
            for c in range(2):
                first = jnp.where(lane == c * step + i, vel[c, x + 1, :, 0:1], first)
                last = jnp.where(lane == c * step + i, vel[c, x + 1, :, depth - 1:depth], last)
                ypack[0, c, pl.ds(x, 1), :] = vel[2 * c, x + 1, 0:1, :]
                ypack[1, c, pl.ds(x, 1), :] = vel[2 * c, x + 1, cols - 1:cols, :]
            return first, last

        loads[k].wait()
        zero = jnp.zeros((cols, LANES), f32)
        ends = lax.fori_loop(0, step, pack, (zero, zero))
        fill = jnp.zeros((LANES - cols, LANES), f32)
        for e in range(2):
            zpack[e, k] = jnp.concatenate([ends[e], fill], axis=0).T[:2 * step]
        mine = pl.ds(k * step, step)
        sides[k] = [
            remote(ypack.at[1, :, mine], yhalo.at[0, :, mine], ys_sem.at[0, k], yr_sem.at[0, k], at(dy=1)),
            remote(ypack.at[0, :, mine], yhalo.at[1, :, mine], ys_sem.at[1, k], yr_sem.at[1, k], at(dy=-1)),
            remote(zpack.at[1, k], zhalo.at[0, k], zs_sem.at[0, k], zr_sem.at[0, k], at(dz=1)),
            remote(zpack.at[0, k], zhalo.at[1, k], zs_sem.at[1, k], zr_sem.at[1, k], at(dz=-1)),
        ]
        for copy in sides[k]:
            copy.start()

    row = lax.broadcasted_iota(jnp.int32, (cols, depth), 0)
    deep = lax.broadcasted_iota(jnp.int32, (cols, depth), 1)

    def second(c, x):
        field = vel[2 * c, x + 1]
        ahead = jnp.where(row == cols - 1, yhalo[1, c, pl.ds(x, 1), :], pltpu.roll(field, cols - 1, 0))
        behind = jnp.where(row == 0, yhalo[0, c, pl.ds(x, 1), :], pltpu.roll(field, 1, 0))
        return ahead - behind

    def third(c, x, i):
        field = vel[c, x + 1]
        here = c * step + i
        after = pltpu.roll(zside[1], LANES - 1 - here, 1)
        before = pltpu.roll(zside[0], lax.rem(LANES - here, LANES), 1)
        after, before = (jnp.concatenate([a] * (depth // LANES), axis=1) for a in (after, before))
        ahead = jnp.where(deep == depth - 1, after, pltpu.roll(field, depth - 1, 1))
        behind = jnp.where(deep == 0, before, pltpu.roll(field, 1, 1))
        return ahead - behind

    def magnitude(x, i):
        total = second(1, x) - third(1, x, i)
        total = total * total
        part = third(0, x, i) - (vel[2, x + 2] - vel[2, x])
        total = total + part * part
        part = (vel[1, x + 2] - vel[1, x]) - second(0, x)
        total = total + part * part
        return jnp.sqrt(1.0 + 0.25 * total)

    def block(target, first, count, k):
        here = pl.ds(pl.multiple_of(me * depth, LANES), depth)
        return remote(
            stage.at[target, pl.ds(first, count)], pencil.at[pl.ds(first, count), :, here],
            as_sem.at[target], ar_sem.at[me, k], (gx, gy, target))

    end = jnp.logical_or(me == 0, me == nz - 1)

    def send_pair(x, k):
        for d in range(1, nz):
            limit = (me + d < nz, me - d >= 0)
            for toward, inside in zip((me + d, me - d), limit):
                go = inside if d == 1 else jnp.logical_and(inside, jnp.logical_not(end))

                @pl.when(go)
                def _():
                    block(toward, x, 2, k).start()

    def level(read):
        return pooled(read, pairs, rows, work)

    def keep(q, lanes, k, value):
        wide = rows // 2
        for j in range(pairs):
            one[k * pairs + j, q * wide:(q + 1) * wide, lanes] = value[j * wide:(j + 1) * wide, :]

    for k in ORDER:
        for copy in sides[k]:
            copy.wait_recv()
        if k == CHUNKS - 1:
            xcopies[1].wait_recv()
        if k == 0:
            xcopies[0].wait_recv()
        fill = jnp.zeros((LANES - 2 * step, LANES), f32)
        for e in range(2):
            zside[e] = jnp.concatenate([zhalo[e, k], fill], axis=0).T[:cols]

        def pair(i, carry):
            for p in range(2):
                x = k * step + 2 * i + p
                value = magnitude(x, 2 * i + p)
                for q in range(nz):
                    stage[q, x] = value[q * rows:(q + 1) * rows, :]

            @pl.when(i > 0)
            def _():
                send_pair(k * step + 2 * i - 2, k)
            return carry

        lax.fori_loop(0, pairs, pair, 0)

        def own(q, carry):
            piece[q * nz + me, k] = level(lambda p: stage[q, k * step + p])
            return carry

        lax.fori_loop(0, nz, own, 0)
        send_pair((k + 1) * step - 2, k)
        for q in range(nz):
            keep(q, pl.ds(pl.multiple_of(me * half, LANES), half), k, piece[q * nz + me, k])
        for p in range(step):
            pencil[k * step + p, :, pl.ds(pl.multiple_of(me * depth, LANES), depth)] = stage[me, k * step + p]

    def move(j, up, q, s, k):
        here = piece.at[q * nz + s, k]
        return remote(
            here, here, move_sem.at[int(up)], piece_sem.at[q * nz + s, k], (gx, gy, j + 1 if up else j - 1))

    def pass_on(j, q, s, k):
        for up in (True, False):
            came = j not in (q, s) and 0 <= (j + 1 if up else j - 1) < nz and carries(
                nz, j + 1 if up else j - 1, not up, q, s)
            if carries(nz, j, up, q, s) and not came:
                move(j, up, q, s, k).start()

    def rest(j):
        for k in ORDER:
            for q in range(nz):
                pass_on(j, q, j, k)
        if j in (0, nz - 1):
            for k in ORDER:
                for d in range(2, nz):
                    block(d if j == 0 else j - d, k * step, step, k).start()
        for _, q, s, turn in events(nz, j):
            k = ORDER[turn]
            lanes = pl.ds(s * half, half)
            if q == j:
                there = pl.ds(s * depth, depth)
                box = pencil.at[pl.ds(k * step, step), :, there]
                remote(stage.at[s, pl.ds(k * step, step)], box, as_sem.at[s], ar_sem.at[s, k], (gx, gy, s)).wait_recv()
                value = level(lambda p: pencil[k * step + p, :, there])
                piece[q * nz + s, k] = value
                keep(q, lanes, k, value)
                pass_on(j, q, s, k)
            else:
                here = piece.at[q * nz + s, k]
                remote(here, here, move_sem.at[0], piece_sem.at[q * nz + s, k], (gx, gy, (j + 1) % nz)).wait_recv()
                pass_on(j, q, s, k)
                keep(q, lanes, k, piece[q * nz + s, k])
        for up in (True, False):
            count = sum(carries(nz, j, up, q, s) for q, s in blocks(nz))
            if count:
                sent = piece.at[pl.ds(0, count)]
                other = j + 1 if up else j - 1
                remote(sent, sent, move_sem.at[int(up)], piece_sem.at[0, 0], (gx, gy, other)).wait_send()

    for j in range(nz):
        pl.when(me == j)(functools.partial(rest, j))

    for copy in xcopies + [c for k in ORDER for c in sides[k]]:
        copy.wait_send()
    for p in range(nz):
        @pl.when(p != me)
        def _():
            block(p, 0, planes, 0).wait_send()


def finish(pencil_in, one_in, pencil, one, two, three, four, five, two_buf, three_buf, four_buf, a, b, c, d, sem):
    copies = [
        pltpu.make_async_copy(pencil_in, pencil, sem.at[0]),
        pltpu.make_async_copy(one_in, one, sem.at[1]),
    ]
    for copy in copies:
        copy.start()
    source = one_in
    for buf, work, target in (
        (two_buf, a, None), (three_buf, b, three), (four_buf, c, four), (None, d, five)
    ):
        planes, size, _ = source.shape
        planes = planes // 2
        value = pooled(lambda i: source[i], planes, size, work)
        size = size // 2
        if buf is None:
            for j in range(size):
                for i in range(planes):
                    target[j, i:i + 1, :] = value[i * size + j:i * size + j + 1, :]
            break
        for i in range(planes):
            buf[i] = value[i * size:(i + 1) * size, :]
        if target is None:
            copies.append(pltpu.make_async_copy(buf, two, sem.at[2]))
            copies[-1].start()
        else:
            for j in range(size):
                target[j] = buf[:, j, :]
        source = buf
    for copy in copies:
        copy.wait()


def on_device(velocity):
    nx, ny, nz = (lax.axis_size(a) for a in ("gx", "gy", "gz"))
    _, planes, cols, depth = velocity.shape
    full = depth * nz
    step = planes // CHUNKS
    f32 = jnp.float32

    def level(k):
        return jax.ShapeDtypeStruct((planes >> k, cols >> k, full >> k), f32)

    def flipped(k):
        return jax.ShapeDtypeStruct((cols >> k, planes >> k, full >> k), f32)

    def work(lines, depth):
        return pltpu.VMEM((pl.cdiv(depth, LANES), lines, LANES), f32)

    def paired(k):
        return work((planes >> k + 1) * (cols >> k), full >> k)

    vmem = pl.BlockSpec(memory_space=pltpu.VMEM)
    anywhere = pl.BlockSpec(memory_space=pl.ANY)
    dma = pltpu.SemaphoreType.DMA
    first = pl.pallas_call(
        functools.partial(kernel, (nx, ny, nz)),
        out_shape=(jax.ShapeDtypeStruct((planes, cols // nz, full), f32), level(1)),
        in_specs=[pl.BlockSpec(memory_space=pltpu.HBM)],
        out_specs=(vmem, vmem),
        scratch_shapes=[
            pltpu.VMEM((3, planes + 2, cols, depth), f32),
            pltpu.VMEM((2, 2, planes, depth), f32),
            pltpu.VMEM((2, 2, planes, depth), f32),
            pltpu.VMEM((2, CHUNKS, 2 * step, LANES), f32),
            pltpu.VMEM((2, CHUNKS, 2 * step, LANES), f32),
            pltpu.VMEM((2, cols, LANES), f32),
            pltpu.VMEM((nz, planes, cols // nz, depth), f32),
            pltpu.VMEM((nz * nz, CHUNKS, step // 2 * cols // nz // 2, depth // 2), f32),
            work(step // 2 * cols // nz, depth),
            dma((CHUNKS,)), dma((2,)), dma((2,)),
            dma((2, CHUNKS)), dma((2, CHUNKS)), dma((2, CHUNKS)), dma((2, CHUNKS)),
            dma((nz,)), dma((nz, CHUNKS)), dma((2,)), dma((nz * nz, CHUNKS)),
        ],
        compiler_params=pltpu.CompilerParams(
            collective_id=0, has_side_effects=True, vmem_limit_bytes=47 * MIB
        ),
    )(velocity)
    last = pl.pallas_call(
        finish,
        out_shape=tuple(jax.ShapeDtypeStruct(x.shape, f32) for x in first)
        + (level(2), flipped(3), flipped(4), flipped(5)),
        in_specs=[vmem] * 2,
        out_specs=(anywhere,) * 3 + (vmem,) * 3,
        scratch_shapes=[
            *(pltpu.VMEM(level(k).shape, f32) for k in (2, 3, 4)), *(paired(k) for k in (1, 2, 3, 4)), dma((3,))],
        compiler_params=pltpu.CompilerParams(vmem_limit_bytes=8 * MIB),
    )(*first)
    return tuple(last[:3]) + tuple(jnp.transpose(x, (1, 0, 2)) for x in last[3:])


def solution(mesh):
    in_specs = (P(None, "gx", "gy", "gz"),)
    out_specs = (P("gx", ("gy", "gz"), None),) + (P("gx", "gy", None),) * 5
    return jax.shard_map(
        on_device, mesh=mesh, in_specs=in_specs, out_specs=out_specs, check_vma=False
    )
```

```python
import functools

import jax
import jax.numpy as jnp
from jax import lax
from jax.experimental import pallas as pl
from jax.experimental.pallas import tpu as pltpu
from jax.sharding import PartitionSpec as P

MESH = pl.DeviceIdType.MESH
LANES = 128
CHUNKS = 4
ORDER = (1, 2, 3, 0)
LOAD_ORDER = (1, 2, 0, 3)
MIB = 1024 * 1024


def remote(src, dst, send, recv, device):
    return pltpu.make_async_remote_copy(
        src_ref=src, dst_ref=dst, send_sem=send, recv_sem=recv, device_id=device, device_id_type=MESH
    )


def halve_lanes(rows):
    depth = rows.shape[1]
    fine = lax.broadcasted_iota(jnp.int32, (depth, depth // 2), 0)
    coarse = lax.broadcasted_iota(jnp.int32, (depth, depth // 2), 1)
    weight = jnp.where(fine // 2 == coarse, 0.125, 0.0).astype(jnp.bfloat16)
    high = rows.astype(jnp.bfloat16)
    rest = rows - high.astype(jnp.float32)
    low = rest.astype(jnp.bfloat16)
    last = (rest - low.astype(jnp.float32)).astype(jnp.bfloat16)

    def dot(a):
        return jnp.dot(a, weight, preferred_element_type=jnp.float32)

    return dot(high) + (dot(low) + dot(last))


def pooled(read, count, size, work):
    tiles = work.shape[0]
    for i in range(count):
        value = read(2 * i) + read(2 * i + 1)
        depth = value.shape[1]
        for t in range(tiles):
            wide = min(LANES, depth - t * LANES)
            work[t, i * size:(i + 1) * size, :wide] = value[:, t * LANES:t * LANES + wide]
    lines = count * size // 2
    parts = [
        work[t, pl.ds(0, lines, stride=2), :] + work[t, pl.ds(1, lines, stride=2), :] for t in range(tiles)]
    return halve_lanes(jnp.concatenate(parts, axis=1)[:, :depth])


def arrivals(n):
    coming = [[]]
    small = 0.5 / CHUNKS
    for j in range(n - 1):
        sends = []
        for k in range(CHUNKS):
            sends.append((2.5 * k, 1.0, (True, j, n - 1, k)))
            sends += [(2.5 * k + 2.0, small, (False, j, q, k)) for q in range(j + 1)]
        between = [(True, j, q, k) for q in range(j + 1, n - 1) for k in range(CHUNKS)]
        relays = [i for i, (_, (mags, _, q, _)) in enumerate(coming[j]) if mags and q == n - 1]
        if not relays:
            sends += [(10.0, 1.0, item) for item in between]
        for i, (time, (mags, s, q, k)) in enumerate(coming[j]):
            time = max(time, 10.0)
            sends.append((time, 1.0 if mags and q != j else small, (mags and q != j, s, q, k)))
            if relays and i == relays[-1]:
                sends += [(time, 1.0, item) for item in between]
        now, there = 0.0, []
        for ready, size, item in sends:
            now = max(now, ready) + 4.2 * size
            there.append((now + 2.0, item))
        coming.append(there)
    return coming


def schedule(n, j):
    coming = arrivals(n)
    events = [(time, True) + item for time, item in coming[j]]
    for time, (mags, s, q, k) in coming[n - 1 - j]:
        events.append((time, False, mags, n - 1 - s, n - 1 - q, k))
    return [e[1:] for e in sorted(events, key=lambda e: e[0])]


def slots(n, j):
    pairs = [(s, q) for s in range(j) for q in range(j + 1, n)]
    pairs += [(s, q) for s in range(j + 1, n) for q in range(j)]
    return {pair: i for i, pair in enumerate(pairs)}


def kernel(
    sizes, vel_hbm, pencil, one,
    vel, ypack, yhalo, zpack, zhalo, zside, stage, transit, piece, work,
    load_sem, xs_sem, xr_sem, ys_sem, yr_sem, zs_sem, zr_sem, mag_sem, ar_sem, tr_sem, move_sem, piece_sem,
):
    nx, ny, nz = sizes
    gx, gy, me = lax.axis_index("gx"), lax.axis_index("gy"), lax.axis_index("gz")
    _, planes, cols, depth = vel_hbm.shape
    rows = cols // nz
    half = depth // 2
    step = planes // CHUNKS
    pairs = step // 2
    group = pairs * rows // 2
    f32 = jnp.float32

    def at(dx=0, dy=0, dz=0):
        return (lax.rem(gx + dx + nx, nx), lax.rem(gy + dy + ny, ny), lax.rem(me + dz + nz, nz))

    barrier = pltpu.get_barrier_semaphore()
    friends = [at(dx=1), at(dx=-1), at(dy=1), at(dy=-1)] + [at(dz=d) for d in range(1, nz)]
    for friend in friends:
        pl.semaphore_signal(barrier, inc=1, device_id=friend, device_id_type=MESH)

    loads = {}
    for k in LOAD_ORDER:
        loads[k] = pltpu.make_async_copy(
            vel_hbm.at[:, pl.ds(k * step, step)], vel.at[:, pl.ds(1 + k * step, step)], load_sem.at[k])
        loads[k].start()
    pl.semaphore_wait(barrier, len(friends))

    xcopies = [
        remote(vel_hbm.at[pl.ds(1, 2), planes - 1], vel.at[pl.ds(1, 2), 0], xs_sem.at[0], xr_sem.at[0], at(dx=1)),
        remote(vel_hbm.at[pl.ds(1, 2), 0], vel.at[pl.ds(1, 2), planes + 1], xs_sem.at[1], xr_sem.at[1], at(dx=-1)),
    ]
    for copy in xcopies:
        copy.start()

    lane = lax.broadcasted_iota(jnp.int32, (cols, LANES), 1)
    sides = {}
    for k in ORDER:
        def pack(i, carry):
            first, last = carry
            x = k * step + i
            for c in range(2):
                first = jnp.where(lane == c * step + i, vel[c, x + 1, :, 0:1], first)
                last = jnp.where(lane == c * step + i, vel[c, x + 1, :, depth - 1:depth], last)
                ypack[0, c, pl.ds(x, 1), :] = vel[2 * c, x + 1, 0:1, :]
                ypack[1, c, pl.ds(x, 1), :] = vel[2 * c, x + 1, cols - 1:cols, :]
            return first, last

        loads[k].wait()
        zero = jnp.zeros((cols, LANES), f32)
        ends = lax.fori_loop(0, step, pack, (zero, zero))
        fill = jnp.zeros((LANES - cols, LANES), f32)
        for e in range(2):
            zpack[e, k] = jnp.concatenate([ends[e], fill], axis=0).T[:2 * step]
        mine = pl.ds(k * step, step)
        sides[k] = [
            remote(ypack.at[1, :, mine], yhalo.at[0, :, mine], ys_sem.at[0, k], yr_sem.at[0, k], at(dy=1)),
            remote(ypack.at[0, :, mine], yhalo.at[1, :, mine], ys_sem.at[1, k], yr_sem.at[1, k], at(dy=-1)),
            remote(zpack.at[1, k], zhalo.at[0, k], zs_sem.at[0, k], zr_sem.at[0, k], at(dz=1)),
            remote(zpack.at[0, k], zhalo.at[1, k], zs_sem.at[1, k], zr_sem.at[1, k], at(dz=-1)),
        ]
        for copy in sides[k]:
            copy.start()

    row = lax.broadcasted_iota(jnp.int32, (cols, depth), 0)
    deep = lax.broadcasted_iota(jnp.int32, (cols, depth), 1)

    def second(c, x):
        field = vel[2 * c, x + 1]
        ahead = jnp.where(row == cols - 1, yhalo[1, c, pl.ds(x, 1), :], pltpu.roll(field, cols - 1, 0))
        behind = jnp.where(row == 0, yhalo[0, c, pl.ds(x, 1), :], pltpu.roll(field, 1, 0))
        return ahead - behind

    def third(c, x, i):
        field = vel[c, x + 1]
        here = c * step + i
        after = pltpu.roll(zside[1], LANES - 1 - here, 1)
        before = pltpu.roll(zside[0], lax.rem(LANES - here, LANES), 1)
        after, before = (jnp.concatenate([a] * (depth // LANES), axis=1) for a in (after, before))
        ahead = jnp.where(deep == depth - 1, after, pltpu.roll(field, depth - 1, 1))
        behind = jnp.where(deep == 0, before, pltpu.roll(field, 1, 1))
        return ahead - behind

    def magnitude(x, i):
        total = second(1, x) - third(1, x, i)
        total = total * total
        part = third(0, x, i) - (vel[2, x + 2] - vel[2, x])
        total = total + part * part
        part = (vel[1, x + 2] - vel[1, x]) - second(0, x)
        total = total + part * part
        return jnp.sqrt(1.0 + 0.25 * total)

    def landing(j, s, q, where):
        if q == j:
            return pencil.at[where, :, pl.ds(s * depth, depth)]
        return transit.at[slots(nz, j)[s, q], where]

    def send_pair(x, k):
        where = pl.ds(x, 2)
        own = pl.ds(pl.multiple_of(me * depth, LANES), depth)
        for up in (True, False):
            target = nz - 1 if up else 0
            other = me + 1 if up else me - 1
            slot = me * (nz - 2 - me) + nz - 3 - me if up else (me - 1) * (nz - me)

            @pl.when(jnp.logical_and(other == target, me != target))
            def _():
                remote(stage.at[target, where], pencil.at[where, :, own],
                       mag_sem.at[int(up), 0], ar_sem.at[me, k], (gx, gy, other)).start()

            @pl.when(jnp.logical_and(other != target, me != target))
            def _():
                remote(stage.at[target, where], transit.at[slot, where],
                       mag_sem.at[int(up), 0], tr_sem.at[slot, k], (gx, gy, other)).start()

    def level(read):
        return pooled(read, pairs, rows, work)

    def keep(q, lanes, k, value):
        wide = rows // 2
        for j in range(pairs):
            one[k * pairs + j, q * wide:(q + 1) * wide, lanes] = value[j * wide:(j + 1) * wide, :]

    def move(j, up, q, s, k):
        here = piece.at[q * nz + s, k]
        return remote(
            here, here, move_sem.at[int(up)], piece_sem.at[q * nz + s, k], (gx, gy, j + 1 if up else j - 1))

    for k in ORDER:
        for copy in sides[k]:
            copy.wait_recv()
        if k == CHUNKS - 1:
            xcopies[1].wait_recv()
        if k == 0:
            xcopies[0].wait_recv()
        fill = jnp.zeros((LANES - 2 * step, LANES), f32)
        for e in range(2):
            zside[e] = jnp.concatenate([zhalo[e, k], fill], axis=0).T[:cols]

        def pair(i, carry):
            for p in range(2):
                x = k * step + 2 * i + p
                value = magnitude(x, 2 * i + p)
                for q in range(nz):
                    stage[q, x] = value[q * rows:(q + 1) * rows, :]

            @pl.when(i > 0)
            def _():
                send_pair(k * step + 2 * i - 2, k)
            return carry

        lax.fori_loop(0, pairs, pair, 0)

        def own(q, carry):
            piece[q * nz + me, k] = level(lambda p: stage[q, k * step + p])
            return carry

        lax.fori_loop(0, nz, own, 0)
        send_pair((k + 1) * step - 2, k)
        for q in range(nz):
            keep(q, pl.ds(pl.multiple_of(me * half, LANES), half), k, piece[q * nz + me, k])
        for p in range(step):
            pencil[k * step + p, :, pl.ds(pl.multiple_of(me * depth, LANES), depth)] = stage[me, k * step + p]
        for q in range(nz):
            @pl.when(jnp.logical_and(me < nz - 1, me >= q))
            def _():
                move(me, True, q, me, k).start()

            @pl.when(jnp.logical_and(me > 0, me <= q))
            def _():
                move(me, False, q, me, k).start()

    def rest(j):
        sent = ({}, {})

        def mags(up, s, q, turn):
            k = ORDER[turn]
            where = pl.ds(k * step, step)
            other = j + 1 if up else j - 1
            source = stage.at[q, where] if s == j else transit.at[slots(nz, j)[s, q], where]
            arrived = ar_sem.at[s, k] if q == other else tr_sem.at[slots(nz, other)[s, q], k]
            row = sent[up].setdefault((s, q), len(sent[up]))
            return remote(source, landing(other, s, q, where), mag_sem.at[int(up), row], arrived, (gx, gy, other))

        def between(up):
            for q in range(j + 1, nz - 1) if up else reversed(range(1, j)):
                for turn in range(CHUNKS):
                    mags(up, j, q, turn).start()

        events = schedule(nz, j)
        last = {}
        for up, far in ((True, nz - 1), (False, 0)):
            if j != far:
                sent[up][j, far] = 0
                waiting = [i for i, (e, whole, _, q, _) in enumerate(events) if e == up and whole and q == far]
                if waiting:
                    last[waiting[-1]] = up
                else:
                    between(up)
        for i, (up, whole, s, q, turn) in enumerate(events):
            k = ORDER[turn]
            more = j < nz - 1 if up else j > 0
            before = (gx, gy, j - 1 if up else j + 1)
            here = piece.at[q * nz + s, k]
            if whole:
                where = pl.ds(k * step, step)
                box = landing(j, s, q, where)
                arrived = ar_sem.at[s, k] if q == j else tr_sem.at[slots(nz, j)[s, q], k]
                remote(box, box, mag_sem.at[0, 0], arrived, before).wait_recv()
                if q != j:
                    mags(up, s, q, turn).start()
                    slot = slots(nz, j)[s, q]
                    value = level(lambda p: transit[slot, k * step + p])
                else:
                    value = level(lambda p: pencil[k * step + p, :, pl.ds(s * depth, depth)])
                    if more:
                        piece[q * nz + s, k] = value
            else:
                remote(here, here, move_sem.at[0], piece_sem.at[q * nz + s, k], before).wait_recv()
                if more:
                    move(j, up, q, s, k).start()
                value = piece[q * nz + s, k]
            keep(q, pl.ds(s * half, half), k, value)
            if whole and q == j and more:
                move(j, up, q, s, k).start()
            if i in last:
                between(last[i])
        for up in (True, False):
            other = (gx, gy, j + 1 if up else j - 1)
            for row in sent[up].values():
                remote(stage.at[0], stage.at[0], mag_sem.at[int(up), row], ar_sem.at[0, 0], other).wait_send()
            count = (j + 1) ** 2 if up else (nz - j) ** 2
            if j != (nz - 1 if up else 0):
                moved = piece.at[pl.ds(0, count)]
                remote(moved, moved, move_sem.at[int(up)], piece_sem.at[0, 0], other).wait_send()

    for j in range(nz):
        pl.when(me == j)(functools.partial(rest, j))

    for copy in xcopies + [c for k in ORDER for c in sides[k]]:
        copy.wait_send()


def finish(pencil_in, one_in, pencil, one, two, three, four, five, two_buf, three_buf, four_buf, a, b, c, d, sem):
    copies = [
        pltpu.make_async_copy(pencil_in, pencil, sem.at[0]),
        pltpu.make_async_copy(one_in, one, sem.at[1]),
    ]
    for copy in copies:
        copy.start()
    source = one_in
    for buf, work, target in (
        (two_buf, a, None), (three_buf, b, three), (four_buf, c, four), (None, d, five)
    ):
        planes, size, _ = source.shape
        planes = planes // 2
        value = pooled(lambda i: source[i], planes, size, work)
        size = size // 2
        if buf is None:
            for j in range(size):
                for i in range(planes):
                    target[j, i:i + 1, :] = value[i * size + j:i * size + j + 1, :]
            break
        for i in range(planes):
            buf[i] = value[i * size:(i + 1) * size, :]
        if target is None:
            copies.append(pltpu.make_async_copy(buf, two, sem.at[2]))
            copies[-1].start()
        else:
            for j in range(size):
                target[j] = buf[:, j, :]
        source = buf
    for copy in copies:
        copy.wait()


def on_device(velocity):
    nx, ny, nz = (lax.axis_size(a) for a in ("gx", "gy", "gz"))
    _, planes, cols, depth = velocity.shape
    full = depth * nz
    step = planes // CHUNKS
    relayed = max(1, *(len(slots(nz, j)) for j in range(nz)))
    passing = max((j + 1) * (nz - 1 - j) for j in range(nz))
    f32 = jnp.float32

    def level(k):
        return jax.ShapeDtypeStruct((planes >> k, cols >> k, full >> k), f32)

    def flipped(k):
        return jax.ShapeDtypeStruct((cols >> k, planes >> k, full >> k), f32)

    def work(lines, depth):
        return pltpu.VMEM((pl.cdiv(depth, LANES), lines, LANES), f32)

    def paired(k):
        return work((planes >> k + 1) * (cols >> k), full >> k)

    vmem = pl.BlockSpec(memory_space=pltpu.VMEM)
    anywhere = pl.BlockSpec(memory_space=pl.ANY)
    dma = pltpu.SemaphoreType.DMA
    first = pl.pallas_call(
        functools.partial(kernel, (nx, ny, nz)),
        out_shape=(jax.ShapeDtypeStruct((planes, cols // nz, full), f32), level(1)),
        in_specs=[pl.BlockSpec(memory_space=pltpu.HBM)],
        out_specs=(vmem, vmem),
        scratch_shapes=[
            pltpu.VMEM((3, planes + 2, cols, depth), f32),
            pltpu.VMEM((2, 2, planes, depth), f32),
            pltpu.VMEM((2, 2, planes, depth), f32),
            pltpu.VMEM((2, CHUNKS, 2 * step, LANES), f32),
            pltpu.VMEM((2, CHUNKS, 2 * step, LANES), f32),
            pltpu.VMEM((2, cols, LANES), f32),
            pltpu.VMEM((nz, planes, cols // nz, depth), f32),
            pltpu.VMEM((relayed, planes, cols // nz, depth), f32),
            pltpu.VMEM((nz * nz, CHUNKS, step // 2 * cols // nz // 2, depth // 2), f32),
            work(step // 2 * cols // nz, depth),
            dma((CHUNKS,)), dma((2,)), dma((2,)),
            dma((2, CHUNKS)), dma((2, CHUNKS)), dma((2, CHUNKS)), dma((2, CHUNKS)),
            dma((2, passing)), dma((nz, CHUNKS)), dma((relayed, CHUNKS)), dma((2,)), dma((nz * nz, CHUNKS)),
        ],
        compiler_params=pltpu.CompilerParams(
            collective_id=0, has_side_effects=True, vmem_limit_bytes=47 * MIB
        ),
    )(velocity)
    last = pl.pallas_call(
        finish,
        out_shape=tuple(jax.ShapeDtypeStruct(x.shape, f32) for x in first)
        + (level(2), flipped(3), flipped(4), flipped(5)),
        in_specs=[vmem] * 2,
        out_specs=(anywhere,) * 3 + (vmem,) * 3,
        scratch_shapes=[
            *(pltpu.VMEM(level(k).shape, f32) for k in (2, 3, 4)), *(paired(k) for k in (1, 2, 3, 4)), dma((3,))],
        compiler_params=pltpu.CompilerParams(vmem_limit_bytes=8 * MIB),
    )(*first)
    return tuple(last[:3]) + tuple(jnp.transpose(x, (1, 0, 2)) for x in last[3:])


def solution(mesh):
    in_specs = (P(None, "gx", "gy", "gz"),)
    out_specs = (P("gx", ("gy", "gz"), None),) + (P("gx", "gy", None),) * 5
    return jax.shard_map(
        on_device, mesh=mesh, in_specs=in_specs, out_specs=out_specs, check_vma=False
    )
```

```python
import functools

import jax
import jax.numpy as jnp
from jax import lax
from jax.experimental import pallas as pl
from jax.experimental.pallas import tpu as pltpu
from jax.sharding import PartitionSpec as P

MESH = pl.DeviceIdType.MESH
LANES = 128
CHUNKS = 4
ORDER = (1, 2, 3, 0)
LOAD_ORDER = (1, 2, 0, 3)
MIB = 1024 * 1024


def remote(src, dst, send, recv, device):
    return pltpu.make_async_remote_copy(
        src_ref=src, dst_ref=dst, send_sem=send, recv_sem=recv, device_id=device, device_id_type=MESH
    )


def halve_lanes(rows):
    depth = rows.shape[1]
    fine = lax.broadcasted_iota(jnp.int32, (depth, depth // 2), 0)
    coarse = lax.broadcasted_iota(jnp.int32, (depth, depth // 2), 1)
    weight = jnp.where(fine // 2 == coarse, 0.125, 0.0).astype(jnp.bfloat16)
    high = rows.astype(jnp.bfloat16)
    rest = rows - high.astype(jnp.float32)
    low = rest.astype(jnp.bfloat16)
    last = (rest - low.astype(jnp.float32)).astype(jnp.bfloat16)

    def dot(a):
        return jnp.dot(a, weight, preferred_element_type=jnp.float32)

    return dot(high) + (dot(low) + dot(last))


def pooled(read, count, size, work):
    tiles = work.shape[0]
    for i in range(count):
        value = read(2 * i) + read(2 * i + 1)
        depth = value.shape[1]
        for t in range(tiles):
            wide = min(LANES, depth - t * LANES)
            work[t, i * size:(i + 1) * size, :wide] = value[:, t * LANES:t * LANES + wide]
    lines = count * size // 2
    parts = [
        work[t, pl.ds(0, lines, stride=2), :] + work[t, pl.ds(1, lines, stride=2), :] for t in range(tiles)]
    return halve_lanes(jnp.concatenate(parts, axis=1)[:, :depth])


def ahead(n, s, q, k):
    return k == CHUNKS - 1 and abs(q - s) > 1 and 0 < q < n - 1


def arrivals(n):
    coming = [[]]
    small = 0.5 / CHUNKS
    for j in range(n - 1):
        sends = []
        for k in range(CHUNKS):
            sends.append((2.5 * k, 1.0, (True, j, n - 1, k)))
            sends += [(2.5 * k + 2.0, small, (False, j, q, k)) for q in range(j + 1)]
        between = [(True, j, q, k) for q in range(j + 1, n - 1) for k in range(CHUNKS)]
        relays = [i for i, (_, (mags, _, q, _)) in enumerate(coming[j]) if mags and q == n - 1]
        if not relays:
            sends += [(10.0, 1.0, item) for item in between]
        for i, (time, (mags, s, q, k)) in enumerate(coming[j]):
            time = max(time, 10.0)
            if mags and q == j + 1 and ahead(n, s, q, k):
                sends.append((time, small, (False, s, q, k)))
            if not mags or q != j or not ahead(n, s, q, k):
                sends.append((time, 1.0 if mags and q != j else small, (mags and q != j, s, q, k)))
            if relays and i == relays[-1]:
                sends += [(time, 1.0, item) for item in between]
        now, there = 0.0, []
        for ready, size, item in sends:
            now = max(now, ready) + 4.2 * size
            there.append((now + 2.0, item))
        coming.append(there)
    return coming


def schedule(n, j):
    coming = arrivals(n)
    events = [(time, True) + item for time, item in coming[j]]
    for time, (mags, s, q, k) in coming[n - 1 - j]:
        events.append((time, False, mags, n - 1 - s, n - 1 - q, k))
    return [e[1:] for e in sorted(events, key=lambda e: e[0])]


def slots(n, j):
    pairs = [(s, q) for s in range(j) for q in range(j + 1, n)]
    pairs += [(s, q) for s in range(j + 1, n) for q in range(j)]
    return {pair: i for i, pair in enumerate(pairs)}


def kernel(
    sizes, vel_hbm, pencil, one,
    vel, ypack, yhalo, zpack, zhalo, zside, stage, transit, piece, work,
    load_sem, xs_sem, xr_sem, ys_sem, yr_sem, zs_sem, zr_sem, mag_sem, ar_sem, tr_sem, move_sem, piece_sem,
):
    nx, ny, nz = sizes
    gx, gy, me = lax.axis_index("gx"), lax.axis_index("gy"), lax.axis_index("gz")
    _, planes, cols, depth = vel_hbm.shape
    rows = cols // nz
    half = depth // 2
    step = planes // CHUNKS
    pairs = step // 2
    group = pairs * rows // 2
    f32 = jnp.float32

    def at(dx=0, dy=0, dz=0):
        return (lax.rem(gx + dx + nx, nx), lax.rem(gy + dy + ny, ny), lax.rem(me + dz + nz, nz))

    barrier = pltpu.get_barrier_semaphore()
    friends = [at(dx=1), at(dx=-1), at(dy=1), at(dy=-1), at(dz=1), at(dz=-1)]
    for friend in friends:
        pl.semaphore_signal(barrier, inc=1, device_id=friend, device_id_type=MESH)

    loads = {}
    for k in LOAD_ORDER:
        loads[k] = pltpu.make_async_copy(
            vel_hbm.at[:, pl.ds(k * step, step)], vel.at[:, pl.ds(1 + k * step, step)], load_sem.at[k])
        loads[k].start()
    xcopies = [
        remote(vel_hbm.at[pl.ds(1, 2), planes - 1], vel.at[pl.ds(1, 2), 0], xs_sem.at[0], xr_sem.at[0], at(dx=1)),
        remote(vel_hbm.at[pl.ds(1, 2), 0], vel.at[pl.ds(1, 2), planes + 1], xs_sem.at[1], xr_sem.at[1], at(dx=-1)),
    ]
    lane = lax.broadcasted_iota(jnp.int32, (cols, LANES), 1)
    sides = {}
    for k in ORDER:
        def pack(i, carry):
            first, last = carry
            x = k * step + i
            for c in range(2):
                first = jnp.where(lane == c * step + i, vel[c, x + 1, :, 0:1], first)
                last = jnp.where(lane == c * step + i, vel[c, x + 1, :, depth - 1:depth], last)
                ypack[0, c, pl.ds(x, 1), :] = vel[2 * c, x + 1, 0:1, :]
                ypack[1, c, pl.ds(x, 1), :] = vel[2 * c, x + 1, cols - 1:cols, :]
            return first, last

        loads[k].wait()
        zero = jnp.zeros((cols, LANES), f32)
        ends = lax.fori_loop(0, step, pack, (zero, zero))
        fill = jnp.zeros((LANES - cols, LANES), f32)
        for e in range(2):
            zpack[e, k] = jnp.concatenate([ends[e], fill], axis=0).T[:2 * step]
        if k == ORDER[0]:
            pl.semaphore_wait(barrier, len(friends))
        mine = pl.ds(k * step, step)
        sides[k] = [
            remote(ypack.at[1, :, mine], yhalo.at[0, :, mine], ys_sem.at[0, k], yr_sem.at[0, k], at(dy=1)),
            remote(ypack.at[0, :, mine], yhalo.at[1, :, mine], ys_sem.at[1, k], yr_sem.at[1, k], at(dy=-1)),
            remote(zpack.at[1, k], zhalo.at[0, k], zs_sem.at[0, k], zr_sem.at[0, k], at(dz=1)),
            remote(zpack.at[0, k], zhalo.at[1, k], zs_sem.at[1, k], zr_sem.at[1, k], at(dz=-1)),
        ]
        for copy in sides[k] + (xcopies if k == ORDER[0] else []):
            copy.start()

    row = lax.broadcasted_iota(jnp.int32, (cols, depth), 0)
    deep = lax.broadcasted_iota(jnp.int32, (cols, depth), 1)

    def second(c, x):
        field = vel[2 * c, x + 1]
        ahead = jnp.where(row == cols - 1, yhalo[1, c, pl.ds(x, 1), :], pltpu.roll(field, cols - 1, 0))
        behind = jnp.where(row == 0, yhalo[0, c, pl.ds(x, 1), :], pltpu.roll(field, 1, 0))
        return ahead - behind

    def third(c, x, i):
        field = vel[c, x + 1]
        here = c * step + i
        after = pltpu.roll(zside[1], LANES - 1 - here, 1)
        before = pltpu.roll(zside[0], lax.rem(LANES - here, LANES), 1)
        after, before = (jnp.concatenate([a] * (depth // LANES), axis=1) for a in (after, before))
        ahead = jnp.where(deep == depth - 1, after, pltpu.roll(field, depth - 1, 1))
        behind = jnp.where(deep == 0, before, pltpu.roll(field, 1, 1))
        return ahead - behind

    def magnitude(x, i):
        total = second(1, x) - third(1, x, i)
        total = total * total
        part = third(0, x, i) - (vel[2, x + 2] - vel[2, x])
        total = total + part * part
        part = (vel[1, x + 2] - vel[1, x]) - second(0, x)
        total = total + part * part
        return jnp.sqrt(1.0 + 0.25 * total)

    def landing(j, s, q, where):
        if q == j:
            return pencil.at[where, :, pl.ds(s * depth, depth)]
        return transit.at[slots(nz, j)[s, q], where]

    def send_pair(x, k):
        where = pl.ds(x, 2)
        own = pl.ds(pl.multiple_of(me * depth, LANES), depth)
        for up in (True, False):
            target = nz - 1 if up else 0
            other = me + 1 if up else me - 1
            slot = me * (nz - 2 - me) + nz - 3 - me if up else (me - 1) * (nz - me)

            @pl.when(jnp.logical_and(other == target, me != target))
            def _():
                remote(stage.at[target, where], pencil.at[where, :, own],
                       mag_sem.at[int(up), 0], ar_sem.at[me, k], (gx, gy, other)).start()

            @pl.when(jnp.logical_and(other != target, me != target))
            def _():
                remote(stage.at[target, where], transit.at[slot, where],
                       mag_sem.at[int(up), 0], tr_sem.at[slot, k], (gx, gy, other)).start()

    def at_piece(q, s, k):
        return (q * nz + s) * CHUNKS + k

    def level(read):
        return pooled(read, pairs, rows, work)

    def keep(q, lanes, k, value):
        wide = rows // 2
        for j in range(pairs):
            one[k * pairs + j, q * wide:(q + 1) * wide, lanes] = value[j * wide:(j + 1) * wide, :]

    def move(j, up, q, s, k):
        here = piece.at[at_piece(q, s, k)]
        return remote(
            here, here, move_sem.at[int(up)], piece_sem.at[q * nz + s, k], (gx, gy, j + 1 if up else j - 1))

    for k in ORDER:
        for copy in sides[k]:
            copy.wait_recv()
        if k == CHUNKS - 1:
            xcopies[1].wait_recv()
        if k == 0:
            xcopies[0].wait_recv()
        fill = jnp.zeros((LANES - 2 * step, LANES), f32)
        for e in range(2):
            zside[e] = jnp.concatenate([zhalo[e, k], fill], axis=0).T[:cols]

        def pair(i, carry):
            for p in range(2):
                x = k * step + 2 * i + p
                value = magnitude(x, 2 * i + p)
                for q in range(nz):
                    stage[q, x] = value[q * rows:(q + 1) * rows, :]

            @pl.when(i > 0)
            def _():
                send_pair(k * step + 2 * i - 2, k)
            return carry

        lax.fori_loop(0, pairs, pair, 0)

        def own(q, carry):
            piece[at_piece(q, me, k)] = level(lambda p: stage[q, k * step + p])
            return carry

        lax.fori_loop(0, nz, own, 0)
        send_pair((k + 1) * step - 2, k)
        for q in range(nz):
            keep(q, pl.ds(pl.multiple_of(me * half, LANES), half), k, piece[at_piece(q, me, k)])
        for p in range(step):
            pencil[k * step + p, :, pl.ds(pl.multiple_of(me * depth, LANES), depth)] = stage[me, k * step + p]
        for q in range(nz):
            @pl.when(jnp.logical_and(me < nz - 1, me >= q))
            def _():
                move(me, True, q, me, k).start()

            @pl.when(jnp.logical_and(me > 0, me <= q))
            def _():
                move(me, False, q, me, k).start()

    def rest(j):
        sent = ({}, {})

        def mags(up, s, q, turn):
            k = ORDER[turn]
            where = pl.ds(k * step, step)
            other = j + 1 if up else j - 1
            source = stage.at[q, where] if s == j else transit.at[slots(nz, j)[s, q], where]
            arrived = ar_sem.at[s, k] if q == other else tr_sem.at[slots(nz, other)[s, q], k]
            row = sent[up].setdefault((s, q), len(sent[up]))
            return remote(source, landing(other, s, q, where), mag_sem.at[int(up), row], arrived, (gx, gy, other))

        def between(up):
            for q in range(j + 1, nz - 1) if up else reversed(range(1, j)):
                for turn in range(CHUNKS):
                    mags(up, j, q, turn).start()

        events = schedule(nz, j)
        last = {}
        for up, far in ((True, nz - 1), (False, 0)):
            if j != far:
                sent[up][j, far] = 0
                waiting = [i for i, (e, whole, _, q, _) in enumerate(events) if e == up and whole and q == far]
                if waiting:
                    last[waiting[-1]] = up
                else:
                    between(up)
        extra = [0, 0]
        for i, (up, whole, s, q, turn) in enumerate(events):
            k = ORDER[turn]
            more = j < nz - 1 if up else j > 0
            before = (gx, gy, j - 1 if up else j + 1)
            here = piece.at[at_piece(q, s, k)]
            if whole:
                where = pl.ds(k * step, step)
                box = landing(j, s, q, where)
                arrived = ar_sem.at[s, k] if q == j else tr_sem.at[slots(nz, j)[s, q], k]
                remote(box, box, mag_sem.at[0, 0], arrived, before).wait_recv()
                if q != j:
                    slot = slots(nz, j)[s, q]
                    first = q == (j + 1 if up else j - 1) and ahead(nz, s, q, turn)
                    if not first:
                        mags(up, s, q, turn).start()
                    value = level(lambda p: transit[slot, k * step + p])
                    if first:
                        piece[at_piece(q, s, k)] = value
                        keep(q, pl.ds(s * half, half), k, value)
                        move(j, up, q, s, k).start()
                        mags(up, s, q, turn).start()
                        extra[up] += 1
                        continue
                elif ahead(nz, s, q, turn):
                    continue
                else:
                    value = level(lambda p: pencil[k * step + p, :, pl.ds(s * depth, depth)])
                    if more:
                        piece[at_piece(q, s, k)] = value
            else:
                remote(here, here, move_sem.at[0], piece_sem.at[q * nz + s, k], before).wait_recv()
                if more:
                    move(j, up, q, s, k).start()
                value = piece[at_piece(q, s, k)]
            keep(q, pl.ds(s * half, half), k, value)
            if whole and q == j and more:
                move(j, up, q, s, k).start()
            if i in last:
                between(last[i])
        for up in (True, False):
            other = (gx, gy, j + 1 if up else j - 1)
            for row in sent[up].values():
                remote(stage.at[0], stage.at[0], mag_sem.at[int(up), row], ar_sem.at[0, 0], other).wait_send()
            count = ((j + 1) ** 2 if up else (nz - j) ** 2) * CHUNKS + extra[up]
            if j != (nz - 1 if up else 0):
                moved = piece.at[pl.ds(0, count)]
                remote(moved, moved, move_sem.at[int(up)], piece_sem.at[0, 0], other).wait_send()

    for j in range(nz):
        pl.when(me == j)(functools.partial(rest, j))

    for copy in xcopies + [c for k in ORDER for c in sides[k]]:
        copy.wait_send()


def finish(pencil_in, one_in, pencil, one, two, three, four, five, two_buf, three_buf, four_buf, a, b, c, d, sem):
    copies = [
        pltpu.make_async_copy(pencil_in, pencil, sem.at[0]),
        pltpu.make_async_copy(one_in, one, sem.at[1]),
    ]
    for copy in copies:
        copy.start()
    source = one_in
    for buf, work, target in (
        (two_buf, a, None), (three_buf, b, three), (four_buf, c, four), (None, d, five)
    ):
        planes, size, _ = source.shape
        planes = planes // 2
        value = pooled(lambda i: source[i], planes, size, work)
        size = size // 2
        if buf is None:
            for j in range(size):
                for i in range(planes):
                    target[j, i:i + 1, :] = value[i * size + j:i * size + j + 1, :]
            break
        for i in range(planes):
            buf[i] = value[i * size:(i + 1) * size, :]
        if target is None:
            copies.append(pltpu.make_async_copy(buf, two, sem.at[2]))
            copies[-1].start()
        else:
            for j in range(size):
                target[j] = buf[:, j, :]
        source = buf
    for copy in copies:
        copy.wait()


def on_device(velocity):
    nx, ny, nz = (lax.axis_size(a) for a in ("gx", "gy", "gz"))
    _, planes, cols, depth = velocity.shape
    full = depth * nz
    step = planes // CHUNKS
    relayed = max(1, *(len(slots(nz, j)) for j in range(nz)))
    passing = max((j + 1) * (nz - 1 - j) for j in range(nz))
    f32 = jnp.float32

    def level(k):
        return jax.ShapeDtypeStruct((planes >> k, cols >> k, full >> k), f32)

    def flipped(k):
        return jax.ShapeDtypeStruct((cols >> k, planes >> k, full >> k), f32)

    def work(lines, depth):
        return pltpu.VMEM((pl.cdiv(depth, LANES), lines, LANES), f32)

    def paired(k):
        return work((planes >> k + 1) * (cols >> k), full >> k)

    vmem = pl.BlockSpec(memory_space=pltpu.VMEM)
    anywhere = pl.BlockSpec(memory_space=pl.ANY)
    dma = pltpu.SemaphoreType.DMA
    first = pl.pallas_call(
        functools.partial(kernel, (nx, ny, nz)),
        out_shape=(jax.ShapeDtypeStruct((planes, cols // nz, full), f32), level(1)),
        in_specs=[pl.BlockSpec(memory_space=pltpu.HBM)],
        out_specs=(vmem, vmem),
        scratch_shapes=[
            pltpu.VMEM((3, planes + 2, cols, depth), f32),
            pltpu.VMEM((2, 2, planes, depth), f32),
            pltpu.VMEM((2, 2, planes, depth), f32),
            pltpu.VMEM((2, CHUNKS, 2 * step, LANES), f32),
            pltpu.VMEM((2, CHUNKS, 2 * step, LANES), f32),
            pltpu.VMEM((2, cols, LANES), f32),
            pltpu.VMEM((nz, planes, cols // nz, depth), f32),
            pltpu.VMEM((relayed, planes, cols // nz, depth), f32),
            pltpu.VMEM((nz * nz * CHUNKS, step // 2 * cols // nz // 2, depth // 2), f32),
            work(step // 2 * cols // nz, depth),
            dma((CHUNKS,)), dma((2,)), dma((2,)),
            dma((2, CHUNKS)), dma((2, CHUNKS)), dma((2, CHUNKS)), dma((2, CHUNKS)),
            dma((2, passing)), dma((nz, CHUNKS)), dma((relayed, CHUNKS)), dma((2,)), dma((nz * nz, CHUNKS)),
        ],
        compiler_params=pltpu.CompilerParams(
            collective_id=0, has_side_effects=True, vmem_limit_bytes=47 * MIB
        ),
    )(velocity)
    last = pl.pallas_call(
        finish,
        out_shape=tuple(jax.ShapeDtypeStruct(x.shape, f32) for x in first)
        + (level(2), flipped(3), flipped(4), flipped(5)),
        in_specs=[vmem] * 2,
        out_specs=(anywhere,) * 3 + (vmem,) * 3,
        scratch_shapes=[
            *(pltpu.VMEM(level(k).shape, f32) for k in (2, 3, 4)), *(paired(k) for k in (1, 2, 3, 4)), dma((3,))],
        compiler_params=pltpu.CompilerParams(vmem_limit_bytes=8 * MIB),
    )(*first)
    return tuple(last[:3]) + tuple(jnp.transpose(x, (1, 0, 2)) for x in last[3:])


def solution(mesh):
    in_specs = (P(None, "gx", "gy", "gz"),)
    out_specs = (P("gx", ("gy", "gz"), None),) + (P("gx", "gy", None),) * 5
    return jax.shard_map(
        on_device, mesh=mesh, in_specs=in_specs, out_specs=out_specs, check_vma=False
    )
```

```python
import functools

import jax
import jax.numpy as jnp
from jax import lax
from jax.experimental import pallas as pl
from jax.experimental.pallas import tpu as pltpu
from jax.sharding import PartitionSpec as P

MESH = pl.DeviceIdType.MESH
LANES = 128
CHUNKS = 4
ORDER = (1, 2, 3, 0)
LOAD_ORDER = (1, 2, 0, 3)
MIB = 1024 * 1024


def remote(src, dst, send, recv, device):
    return pltpu.make_async_remote_copy(
        src_ref=src, dst_ref=dst, send_sem=send, recv_sem=recv, device_id=device, device_id_type=MESH
    )


def halve_lanes(rows):
    depth = rows.shape[1]
    fine = lax.broadcasted_iota(jnp.int32, (depth, depth // 2), 0)
    coarse = lax.broadcasted_iota(jnp.int32, (depth, depth // 2), 1)
    weight = jnp.where(fine // 2 == coarse, 0.125, 0.0).astype(jnp.bfloat16)
    high = rows.astype(jnp.bfloat16)
    rest = rows - high.astype(jnp.float32)
    low = rest.astype(jnp.bfloat16)
    last = (rest - low.astype(jnp.float32)).astype(jnp.bfloat16)

    def dot(a):
        return jnp.dot(a, weight, preferred_element_type=jnp.float32)

    return dot(high) + (dot(low) + dot(last))


def pooled(read, count, size, work):
    tiles = work.shape[0]
    for i in range(count):
        value = read(2 * i) + read(2 * i + 1)
        depth = value.shape[1]
        for t in range(tiles):
            wide = min(LANES, depth - t * LANES)
            work[t, i * size:(i + 1) * size, :wide] = value[:, t * LANES:t * LANES + wide]
    lines = count * size // 2
    parts = [
        work[t, pl.ds(0, lines, stride=2), :] + work[t, pl.ds(1, lines, stride=2), :] for t in range(tiles)]
    return halve_lanes(jnp.concatenate(parts, axis=1)[:, :depth])


def ahead(n, s, q, k):
    return k >= CHUNKS - 2 and abs(q - s) > 1 and 0 < q < n - 1


def arrivals(n):
    coming = [[]]
    small = 0.5 / CHUNKS
    for j in range(n - 1):
        sends = []
        for k in range(CHUNKS):
            sends.append((2.5 * k, 1.0, (True, j, n - 1, k)))
            sends += [(2.5 * k + 2.0, small, (False, j, q, k)) for q in range(j + 1)]
        between = [(True, j, q, k) for q in range(j + 1, n - 1) for k in range(CHUNKS)]
        relays = [i for i, (_, (mags, _, q, _)) in enumerate(coming[j]) if mags and q == n - 1]
        if not relays:
            sends += [(10.0, 1.0, item) for item in between]
        for i, (time, (mags, s, q, k)) in enumerate(coming[j]):
            time = max(time, 10.0)
            if mags and q == j + 1 and ahead(n, s, q, k):
                sends.append((time, small, (False, s, q, k)))
                if k == CHUNKS - 1:
                    sends += [(time, 1.0, (True, s, q, held)) for held in (k - 1, k)]
            elif not mags or q != j or not ahead(n, s, q, k):
                sends.append((time, 1.0 if mags and q != j else small, (mags and q != j, s, q, k)))
            if relays and i == relays[-1]:
                sends += [(time, 1.0, item) for item in between]
        now, there = 0.0, []
        for ready, size, item in sends:
            now = max(now, ready) + 4.2 * size
            there.append((now + 2.0, item))
        coming.append(there)
    return coming


def schedule(n, j):
    coming = arrivals(n)
    events = [(time, True) + item for time, item in coming[j]]
    for time, (mags, s, q, k) in coming[n - 1 - j]:
        events.append((time, False, mags, n - 1 - s, n - 1 - q, k))
    return [e[1:] for e in sorted(events, key=lambda e: e[0])]


def slots(n, j):
    pairs = [(s, q) for s in range(j) for q in range(j + 1, n)]
    pairs += [(s, q) for s in range(j + 1, n) for q in range(j)]
    return {pair: i for i, pair in enumerate(pairs)}


def kernel(
    sizes, vel_hbm, pencil, one,
    vel, ypack, yhalo, zpack, zhalo, zside, stage, transit, piece, work,
    load_sem, xs_sem, xr_sem, ys_sem, yr_sem, zs_sem, zr_sem, mag_sem, ar_sem, tr_sem, move_sem, piece_sem,
):
    nx, ny, nz = sizes
    gx, gy, me = lax.axis_index("gx"), lax.axis_index("gy"), lax.axis_index("gz")
    _, planes, cols, depth = vel_hbm.shape
    rows = cols // nz
    half = depth // 2
    step = planes // CHUNKS
    pairs = step // 2
    group = pairs * rows // 2
    f32 = jnp.float32

    def at(dx=0, dy=0, dz=0):
        return (lax.rem(gx + dx + nx, nx), lax.rem(gy + dy + ny, ny), lax.rem(me + dz + nz, nz))

    barrier = pltpu.get_barrier_semaphore()
    friends = [at(dx=1), at(dx=-1), at(dy=1), at(dy=-1), at(dz=1), at(dz=-1)]
    for friend in friends:
        pl.semaphore_signal(barrier, inc=1, device_id=friend, device_id_type=MESH)

    loads = {}
    for k in LOAD_ORDER:
        loads[k] = pltpu.make_async_copy(
            vel_hbm.at[:, pl.ds(k * step, step)], vel.at[:, pl.ds(1 + k * step, step)], load_sem.at[k])
        loads[k].start()
    xcopies = [
        remote(vel_hbm.at[pl.ds(1, 2), planes - 1], vel.at[pl.ds(1, 2), 0], xs_sem.at[0], xr_sem.at[0], at(dx=1)),
        remote(vel_hbm.at[pl.ds(1, 2), 0], vel.at[pl.ds(1, 2), planes + 1], xs_sem.at[1], xr_sem.at[1], at(dx=-1)),
    ]
    lane = lax.broadcasted_iota(jnp.int32, (cols, LANES), 1)
    sides = {}
    for k in ORDER:
        def pack(i, carry):
            first, last = carry
            x = k * step + i
            for c in range(2):
                first = jnp.where(lane == c * step + i, vel[c, x + 1, :, 0:1], first)
                last = jnp.where(lane == c * step + i, vel[c, x + 1, :, depth - 1:depth], last)
                ypack[0, c, pl.ds(x, 1), :] = vel[2 * c, x + 1, 0:1, :]
                ypack[1, c, pl.ds(x, 1), :] = vel[2 * c, x + 1, cols - 1:cols, :]
            return first, last

        loads[k].wait()
        zero = jnp.zeros((cols, LANES), f32)
        ends = lax.fori_loop(0, step, pack, (zero, zero))
        fill = jnp.zeros((LANES - cols, LANES), f32)
        for e in range(2):
            zpack[e, k] = jnp.concatenate([ends[e], fill], axis=0).T[:2 * step]
        if k == ORDER[0]:
            pl.semaphore_wait(barrier, len(friends))
        mine = pl.ds(k * step, step)
        sides[k] = [
            remote(ypack.at[1, :, mine], yhalo.at[0, :, mine], ys_sem.at[0, k], yr_sem.at[0, k], at(dy=1)),
            remote(ypack.at[0, :, mine], yhalo.at[1, :, mine], ys_sem.at[1, k], yr_sem.at[1, k], at(dy=-1)),
            remote(zpack.at[1, k], zhalo.at[0, k], zs_sem.at[0, k], zr_sem.at[0, k], at(dz=1)),
            remote(zpack.at[0, k], zhalo.at[1, k], zs_sem.at[1, k], zr_sem.at[1, k], at(dz=-1)),
        ]
        for copy in sides[k] + (xcopies if k == ORDER[0] else []):
            copy.start()

    row = lax.broadcasted_iota(jnp.int32, (cols, depth), 0)
    deep = lax.broadcasted_iota(jnp.int32, (cols, depth), 1)

    def second(c, x):
        field = vel[2 * c, x + 1]
        ahead = jnp.where(row == cols - 1, yhalo[1, c, pl.ds(x, 1), :], pltpu.roll(field, cols - 1, 0))
        behind = jnp.where(row == 0, yhalo[0, c, pl.ds(x, 1), :], pltpu.roll(field, 1, 0))
        return ahead - behind

    def third(c, x, i):
        field = vel[c, x + 1]
        here = c * step + i
        after = pltpu.roll(zside[1], LANES - 1 - here, 1)
        before = pltpu.roll(zside[0], lax.rem(LANES - here, LANES), 1)
        after, before = (jnp.concatenate([a] * (depth // LANES), axis=1) for a in (after, before))
        ahead = jnp.where(deep == depth - 1, after, pltpu.roll(field, depth - 1, 1))
        behind = jnp.where(deep == 0, before, pltpu.roll(field, 1, 1))
        return ahead - behind

    def magnitude(x, i):
        total = second(1, x) - third(1, x, i)
        total = total * total
        part = third(0, x, i) - (vel[2, x + 2] - vel[2, x])
        total = total + part * part
        part = (vel[1, x + 2] - vel[1, x]) - second(0, x)
        total = total + part * part
        return jnp.sqrt(1.0 + 0.25 * total)

    def landing(j, s, q, where):
        if q == j:
            return pencil.at[where, :, pl.ds(s * depth, depth)]
        return transit.at[slots(nz, j)[s, q], where]

    def send_pair(x, k):
        where = pl.ds(x, 2)
        own = pl.ds(pl.multiple_of(me * depth, LANES), depth)
        for up in (True, False):
            target = nz - 1 if up else 0
            other = me + 1 if up else me - 1
            slot = me * (nz - 2 - me) + nz - 3 - me if up else (me - 1) * (nz - me)

            @pl.when(jnp.logical_and(other == target, me != target))
            def _():
                remote(stage.at[target, where], pencil.at[where, :, own],
                       mag_sem.at[int(up), 0], ar_sem.at[me, k], (gx, gy, other)).start()

            @pl.when(jnp.logical_and(other != target, me != target))
            def _():
                remote(stage.at[target, where], transit.at[slot, where],
                       mag_sem.at[int(up), 0], tr_sem.at[slot, k], (gx, gy, other)).start()

    def at_piece(q, s, k):
        return (q * nz + s) * CHUNKS + k

    def level(read):
        return pooled(read, pairs, rows, work)

    def keep(q, lanes, k, value):
        wide = rows // 2
        for j in range(pairs):
            one[k * pairs + j, q * wide:(q + 1) * wide, lanes] = value[j * wide:(j + 1) * wide, :]

    def move(j, up, q, s, k):
        here = piece.at[at_piece(q, s, k)]
        return remote(
            here, here, move_sem.at[int(up)], piece_sem.at[q * nz + s, k], (gx, gy, j + 1 if up else j - 1))

    for k in ORDER:
        for copy in sides[k]:
            copy.wait_recv()
        if k == CHUNKS - 1:
            xcopies[1].wait_recv()
        if k == 0:
            xcopies[0].wait_recv()
        fill = jnp.zeros((LANES - 2 * step, LANES), f32)
        for e in range(2):
            zside[e] = jnp.concatenate([zhalo[e, k], fill], axis=0).T[:cols]

        def pair(i, carry):
            for p in range(2):
                x = k * step + 2 * i + p
                value = magnitude(x, 2 * i + p)
                for q in range(nz):
                    stage[q, x] = value[q * rows:(q + 1) * rows, :]

            @pl.when(i > 0)
            def _():
                send_pair(k * step + 2 * i - 2, k)
            return carry

        lax.fori_loop(0, pairs, pair, 0)

        def own(q, carry):
            piece[at_piece(q, me, k)] = level(lambda p: stage[q, k * step + p])
            return carry

        lax.fori_loop(0, nz, own, 0)
        send_pair((k + 1) * step - 2, k)
        for q in range(nz):
            keep(q, pl.ds(pl.multiple_of(me * half, LANES), half), k, piece[at_piece(q, me, k)])
        for p in range(step):
            pencil[k * step + p, :, pl.ds(pl.multiple_of(me * depth, LANES), depth)] = stage[me, k * step + p]
        for q in range(nz):
            @pl.when(jnp.logical_and(me < nz - 1, me >= q))
            def _():
                move(me, True, q, me, k).start()

            @pl.when(jnp.logical_and(me > 0, me <= q))
            def _():
                move(me, False, q, me, k).start()

    def rest(j):
        sent = ({}, {})

        def mags(up, s, q, turn):
            k = ORDER[turn]
            where = pl.ds(k * step, step)
            other = j + 1 if up else j - 1
            source = stage.at[q, where] if s == j else transit.at[slots(nz, j)[s, q], where]
            arrived = ar_sem.at[s, k] if q == other else tr_sem.at[slots(nz, other)[s, q], k]
            row = sent[up].setdefault((s, q), len(sent[up]))
            return remote(source, landing(other, s, q, where), mag_sem.at[int(up), row], arrived, (gx, gy, other))

        def between(up):
            for q in range(j + 1, nz - 1) if up else reversed(range(1, j)):
                for turn in range(CHUNKS):
                    mags(up, j, q, turn).start()

        events = schedule(nz, j)
        last = {}
        for up, far in ((True, nz - 1), (False, 0)):
            if j != far:
                sent[up][j, far] = 0
                waiting = [i for i, (e, whole, _, q, _) in enumerate(events) if e == up and whole and q == far]
                if waiting:
                    last[waiting[-1]] = up
                else:
                    between(up)
        extra = [0, 0]
        for i, (up, whole, s, q, turn) in enumerate(events):
            k = ORDER[turn]
            more = j < nz - 1 if up else j > 0
            before = (gx, gy, j - 1 if up else j + 1)
            here = piece.at[at_piece(q, s, k)]
            if whole:
                where = pl.ds(k * step, step)
                box = landing(j, s, q, where)
                arrived = ar_sem.at[s, k] if q == j else tr_sem.at[slots(nz, j)[s, q], k]
                remote(box, box, mag_sem.at[0, 0], arrived, before).wait_recv()
                if q != j:
                    slot = slots(nz, j)[s, q]
                    first = q == (j + 1 if up else j - 1) and ahead(nz, s, q, turn)
                    if not first:
                        mags(up, s, q, turn).start()
                    value = level(lambda p: transit[slot, k * step + p])
                    if first:
                        piece[at_piece(q, s, k)] = value
                        keep(q, pl.ds(s * half, half), k, value)
                        move(j, up, q, s, k).start()
                        if turn == CHUNKS - 1:
                            mags(up, s, q, turn - 1).start()
                            mags(up, s, q, turn).start()
                        extra[up] += 1
                        continue
                elif ahead(nz, s, q, turn):
                    continue
                else:
                    value = level(lambda p: pencil[k * step + p, :, pl.ds(s * depth, depth)])
                    if more:
                        piece[at_piece(q, s, k)] = value
            else:
                remote(here, here, move_sem.at[0], piece_sem.at[q * nz + s, k], before).wait_recv()
                if more:
                    move(j, up, q, s, k).start()
                value = piece[at_piece(q, s, k)]
            keep(q, pl.ds(s * half, half), k, value)
            if whole and q == j and more:
                move(j, up, q, s, k).start()
            if i in last:
                between(last[i])
        for up in (True, False):
            other = (gx, gy, j + 1 if up else j - 1)
            for row in sent[up].values():
                remote(stage.at[0], stage.at[0], mag_sem.at[int(up), row], ar_sem.at[0, 0], other).wait_send()
            count = ((j + 1) ** 2 if up else (nz - j) ** 2) * CHUNKS + extra[up]
            if j != (nz - 1 if up else 0):
                moved = piece.at[pl.ds(0, count)]
                remote(moved, moved, move_sem.at[int(up)], piece_sem.at[0, 0], other).wait_send()

    for j in range(nz):
        pl.when(me == j)(functools.partial(rest, j))

    for copy in xcopies + [c for k in ORDER for c in sides[k]]:
        copy.wait_send()


def finish(pencil_in, one_in, pencil, one, two, three, four, five, two_buf, three_buf, four_buf, a, b, c, d, sem):
    copies = [
        pltpu.make_async_copy(pencil_in, pencil, sem.at[0]),
        pltpu.make_async_copy(one_in, one, sem.at[1]),
    ]
    for copy in copies:
        copy.start()
    source = one_in
    for buf, work, target in (
        (two_buf, a, None), (three_buf, b, three), (four_buf, c, four), (None, d, five)
    ):
        planes, size, _ = source.shape
        planes = planes // 2
        value = pooled(lambda i: source[i], planes, size, work)
        size = size // 2
        if buf is None:
            for j in range(size):
                for i in range(planes):
                    target[j, i:i + 1, :] = value[i * size + j:i * size + j + 1, :]
            break
        for i in range(planes):
            buf[i] = value[i * size:(i + 1) * size, :]
        if target is None:
            copies.append(pltpu.make_async_copy(buf, two, sem.at[2]))
            copies[-1].start()
        else:
            for j in range(size):
                target[j] = buf[:, j, :]
        source = buf
    for copy in copies:
        copy.wait()


def on_device(velocity):
    nx, ny, nz = (lax.axis_size(a) for a in ("gx", "gy", "gz"))
    _, planes, cols, depth = velocity.shape
    full = depth * nz
    step = planes // CHUNKS
    relayed = max(1, *(len(slots(nz, j)) for j in range(nz)))
    passing = max((j + 1) * (nz - 1 - j) for j in range(nz))
    f32 = jnp.float32

    def level(k):
        return jax.ShapeDtypeStruct((planes >> k, cols >> k, full >> k), f32)

    def flipped(k):
        return jax.ShapeDtypeStruct((cols >> k, planes >> k, full >> k), f32)

    def work(lines, depth):
        return pltpu.VMEM((pl.cdiv(depth, LANES), lines, LANES), f32)

    def paired(k):
        return work((planes >> k + 1) * (cols >> k), full >> k)

    vmem = pl.BlockSpec(memory_space=pltpu.VMEM)
    anywhere = pl.BlockSpec(memory_space=pl.ANY)
    dma = pltpu.SemaphoreType.DMA
    first = pl.pallas_call(
        functools.partial(kernel, (nx, ny, nz)),
        out_shape=(jax.ShapeDtypeStruct((planes, cols // nz, full), f32), level(1)),
        in_specs=[pl.BlockSpec(memory_space=pltpu.HBM)],
        out_specs=(vmem, vmem),
        scratch_shapes=[
            pltpu.VMEM((3, planes + 2, cols, depth), f32),
            pltpu.VMEM((2, 2, planes, depth), f32),
            pltpu.VMEM((2, 2, planes, depth), f32),
            pltpu.VMEM((2, CHUNKS, 2 * step, LANES), f32),
            pltpu.VMEM((2, CHUNKS, 2 * step, LANES), f32),
            pltpu.VMEM((2, cols, LANES), f32),
            pltpu.VMEM((nz, planes, cols // nz, depth), f32),
            pltpu.VMEM((relayed, planes, cols // nz, depth), f32),
            pltpu.VMEM((nz * nz * CHUNKS, step // 2 * cols // nz // 2, depth // 2), f32),
            work(step // 2 * cols // nz, depth),
            dma((CHUNKS,)), dma((2,)), dma((2,)),
            dma((2, CHUNKS)), dma((2, CHUNKS)), dma((2, CHUNKS)), dma((2, CHUNKS)),
            dma((2, passing)), dma((nz, CHUNKS)), dma((relayed, CHUNKS)), dma((2,)), dma((nz * nz, CHUNKS)),
        ],
        compiler_params=pltpu.CompilerParams(
            collective_id=0, has_side_effects=True, vmem_limit_bytes=47 * MIB
        ),
    )(velocity)
    last = pl.pallas_call(
        finish,
        out_shape=tuple(jax.ShapeDtypeStruct(x.shape, f32) for x in first)
        + (level(2), flipped(3), flipped(4), flipped(5)),
        in_specs=[vmem] * 2,
        out_specs=(anywhere,) * 3 + (vmem,) * 3,
        scratch_shapes=[
            *(pltpu.VMEM(level(k).shape, f32) for k in (2, 3, 4)), *(paired(k) for k in (1, 2, 3, 4)), dma((3,))],
        compiler_params=pltpu.CompilerParams(vmem_limit_bytes=8 * MIB),
    )(*first)
    return tuple(last[:3]) + tuple(jnp.transpose(x, (1, 0, 2)) for x in last[3:])


def solution(mesh):
    in_specs = (P(None, "gx", "gy", "gz"),)
    out_specs = (P("gx", ("gy", "gz"), None),) + (P("gx", "gy", None),) * 5
    return jax.shard_map(
        on_device, mesh=mesh, in_specs=in_specs, out_specs=out_specs, check_vma=False
    )
```
